32 devices in a mesh: ctx: 8 (over z, y), head: 4 (over x, core).
Axes of the slice: x: 2, y: 2, z: 4, core: 2. Of those that a mesh axis runs over, the one named last changes fastest.
Arguments:
- queries: bfloat16 [2048, 8192], P('ctx', 'head'), may hold values from -15 to 15
- keys: bfloat16 [2048, 1024], P('ctx'), may hold values from -6 to 6
- values: bfloat16 [2048, 1024], P('ctx'), may hold values from -6 to 6
Outputs:
- attended: bfloat16 [2048, 8192], P('ctx', 'head')
The draws below stay inside these ranges and needn't reach their ends.
All inputs are finite; a program needn't handle non-finite values.
Results may differ from the reference program's by a relative error of at most 0.015.
Values may be sent and summed in bfloat16 or wider, within the bound.
No kernel may reach another device: no remote copies, remote signals or barrier semaphores. Data moves between devices by JAX's collectives and lax.ppermute only.
A program may use at most 128 MiB of HBM per device.

```python
import math
import jax
import jax.numpy as jnp
from jax import lax

H = 64
KVH = 8
HD = 128
TOKENS = 2048


def draw_queries(key, part):
    noise_key = jax.random.fold_in(key, 1)
    base_rows = jax.random.normal(noise_key, (TOKENS, H * HD), jnp.float32)
    drawn = jnp.clip(2.5 * base_rows, -15.0, 15.0)
    return drawn.astype(jnp.bfloat16)


def draw_keys(key, part):
    noise_key = jax.random.fold_in(key, 2)
    base_rows = jax.random.normal(noise_key, (TOKENS, KVH * HD), jnp.float32)
    drawn = jnp.clip(base_rows, -6.0, 6.0)
    return drawn.astype(jnp.bfloat16)


def level_of(own_key, dims, cuts, smallest, high):
    gain, own = 1.0, jax.random.fold_in(own_key, 6)
    for dim, shards_of in cuts:
        heights = jnp.exp(jax.random.uniform(jax.random.fold_in(own, dim), (shards_of,), jnp.float32, smallest / len(cuts), high / len(cuts)))
        gain = gain * jnp.repeat(heights, dims[dim] // shards_of).reshape([-1 if axis == dim else 1 for axis in range(len(dims))])
    return gain


def gaussian(stream_key, extent, scale, limit, cuts=(), kind=jnp.bfloat16):
    gain = level_of(stream_key, extent, cuts, -0.22, 0.18) if cuts else 1.0
    entries = jax.random.normal(stream_key, extent, jnp.float32) * scale * gain
    return jnp.minimum(jnp.maximum(entries, -limit), limit).astype(kind)


def setup_inputs(seed: int = 0) -> dict:
    streams_of = jax.random.split(jax.random.key(seed), 4)
    queries = draw_queries(jax.random.fold_in(streams_of[3], 71), 0)
    keys = draw_keys(jax.random.fold_in(streams_of[3], 71), 0)
    values = gaussian(streams_of[2], (TOKENS, KVH * HD), 1.0, 6.0, ((0, 8),))
    return dict(queries=queries, keys=keys, values=values)


def reference(queries, keys, values):
    group_size = H // KVH
    block_rows = math.gcd(TOKENS, 512)
    block_count = TOKENS // block_rows
    grouped = queries.reshape(TOKENS, KVH, group_size, HD)
    keyed = keys.reshape(TOKENS, KVH, HD).astype(jnp.float32)
    valued = values.reshape(TOKENS, KVH, HD).astype(jnp.float32)
    key_pos = jnp.arange(TOKENS, dtype=jnp.int32)

    def one_block(block_index):
        block_start = (block_index // KVH) * block_rows
        kv_head = block_index % KVH
        zero_index = jnp.zeros((), jnp.int32)
        query_block = lax.dynamic_slice(grouped, (block_start, kv_head, zero_index, zero_index), (block_rows, 1, group_size, HD))[:, 0].astype(jnp.float32)
        key_head = lax.dynamic_slice_in_dim(keyed, kv_head, 1, 1)[:, 0]
        value_head = lax.dynamic_slice_in_dim(valued, kv_head, 1, 1)[:, 0]
        scores = jnp.einsum("qrd,kd->rqk", query_block, key_head, precision=lax.Precision.HIGHEST) * (HD ** -0.5)
        allowed = (block_start + jnp.arange(block_rows, dtype=jnp.int32))[:, None] >= key_pos[None, :]
        scores = jnp.where(allowed, scores, jnp.float32(-1e30))
        row_max = jnp.max(scores, axis=-1)
        weights = jnp.where(allowed, jnp.exp(scores - row_max[..., None]), jnp.float32(0.0))
        totals = jnp.sum(weights, axis=-1)
        rounded = lax.optimization_barrier(weights.astype(jnp.bfloat16)).astype(jnp.float32)
        result = jnp.einsum("rqk,kd->rqd", rounded, value_head, precision=lax.Precision.HIGHEST) / totals[..., None]
        return result.astype(jnp.bfloat16)

    stacked = lax.map(one_block, jnp.arange(block_count * KVH, dtype=jnp.int32))
    stacked = stacked.reshape(block_count, KVH, group_size, block_rows, HD)
    return jnp.transpose(stacked, (0, 3, 1, 2, 4)).reshape(TOKENS, H * HD)
```

```python
import functools
import math

import jax
import jax.numpy as jnp
from jax import lax
from jax.experimental import pallas as pl
from jax.experimental.pallas import tpu as pltpu
from jax.sharding import PartitionSpec as P


H = 64
KVH = 8
HD = 128
BIG = 1e30
VMEM = pl.BlockSpec(memory_space=pltpu.VMEM)
NT = (((1,), (1,)), ((), ()))


def moved(value, target):
    ctx, head = lax.axis_size("ctx"), lax.axis_size("head")
    pairs = []
    for c in range(ctx):
        to = target(c)
        for h in range(head):
            if to is not None:
                pairs.append((c * head + h, to * head + h))
            elif head % 2 == 0:
                pairs.append((c * head + h, c * head + (h ^ 1)))
    return lax.ppermute(value, ("ctx", "head"), pairs)


def attend_kernel(q_ref, *refs, wanted, first, last, rep, heads, unroll, rb):
    kv_refs, refs = refs[: len(wanted)], refs[len(wanted) :]
    place = lax.axis_index("ctx")
    flags = [w(place) for w in wanted]
    if not first:
        m_in, a_in, *refs = refs
    if last:
        (o_ref,) = refs
    else:
        m_out, a_out = refs
    tok = q_ref.shape[0]
    scale = HD**-0.5 * math.log2(math.e)
    ones = jnp.ones((tok, HD), jnp.bfloat16)

    def one(h, r):
        rows = pl.ds(r * rb, rb)
        col = pl.ds(pl.multiple_of(h * HD, HD), HD)
        kcol = pl.multiple_of(h // rep * 2 * HD, 2 * HD)
        q = q_ref[rows, col]
        scores, shifts = [], []
        m_prev = m = None if first else m_in[h, rows]
        for i, kv in enumerate(kv_refs):
            k = kv[:, pl.ds(kcol, HD)]
            s = lax.dot_general(q, k, NT, preferred_element_type=jnp.float32) * scale
            if first:
                t = lax.broadcasted_iota(jnp.int32, s.shape, 0) + r * rb
                u = lax.broadcasted_iota(jnp.int32, s.shape, 1)
                s = jnp.where(t >= u, s, -BIG)
                bias = None
            else:
                bias = jnp.where(flags[i], 0.0, -BIG)
            top = jnp.max(s, axis=1, keepdims=True)
            top = jnp.broadcast_to(top if bias is None else top + bias, (rb, HD))
            m = top if m is None else jnp.maximum(m, top)
            scores.append(s)
            shifts.append(bias)
        acc = None
        for s, bias, kv in zip(scores, shifts, kv_refs):
            shift = m if bias is None else m - bias
            p = jnp.exp2(s - jnp.concatenate([shift] * (tok // HD), axis=1)).astype(jnp.bfloat16)
            v = jnp.concatenate([kv[:, pl.ds(kcol + HD, HD)], ones], axis=1)
            d = jnp.dot(p, v, preferred_element_type=jnp.float32)
            acc = d if acc is None else acc + d
        if not first:
            fade = jnp.exp2(m_prev - m)
            acc = acc + a_in[h, rows] * jnp.concatenate([fade, fade], axis=1)
        if last:
            o_ref[rows, col] = (acc[:, :HD] / acc[:, HD:]).astype(o_ref.dtype)
        else:
            m_out[h, rows] = m
            a_out[h, rows] = acc

    def work():
        def step(t, carry):
            for u in range(unroll):
                for r in range(tok // rb):
                    one(t * unroll + u, r)
            return carry

        lax.fori_loop(0, heads // unroll, step, 0)

    def finish():
        def step(h, carry):
            acc = a_in[h]
            o_ref[:, pl.ds(pl.multiple_of(h * HD, HD), HD)] = (acc[:, :HD] / acc[:, HD:]).astype(o_ref.dtype)
            return carry

        lax.fori_loop(0, heads, step, 0)

    if first:
        work()
        return
    live = functools.reduce(jnp.logical_or, flags)
    pl.when(live)(work)
    if last:
        pl.when(jnp.logical_not(live))(finish)


def attend(wanted, q, kvs, state, rep, last):
    tok, heads = q.shape[0], q.shape[1] // HD
    n, first = len(kvs), state is None
    held = [
        jax.ShapeDtypeStruct((heads, tok, HD), jnp.float32),
        jax.ShapeDtypeStruct((heads, tok, 2 * HD), jnp.float32),
    ]
    unroll = math.gcd(heads, 8)
    rb = math.gcd(tok, 128)
    return pl.pallas_call(
        functools.partial(attend_kernel, wanted=wanted, first=first, last=last, rep=rep, heads=heads, unroll=unroll, rb=rb),
        out_shape=jax.ShapeDtypeStruct(q.shape, q.dtype) if last else held,
        in_specs=[VMEM] * (1 + n + (0 if first else 2)),
        out_specs=VMEM if last else [VMEM, VMEM],
        input_output_aliases={} if first or last else {1 + n: 0, 2 + n: 1},
        compiler_params=pltpu.CompilerParams(vmem_limit_bytes=24 << 20),
        cost_estimate=pl.CostEstimate(
            flops=4 * tok * tok * HD * heads * n, transcendentals=tok * tok * heads * n, bytes_accessed=4 << 20
        ),
    )(q, *kvs, *(() if first else state))


def body(queries, keys, values):
    heads = queries.shape[1] // HD
    group = H // KVH
    kv_count = max(1, heads // group)
    rep = heads // kv_count
    first_col = lax.axis_index("head") * heads // group * HD
    k_own = lax.dynamic_slice_in_dim(keys, first_col, kv_count * HD, 1)
    v_own = lax.dynamic_slice_in_dim(values, first_col, kv_count * HD, 1)
    parts = []
    for g in range(kv_count):
        parts += [k_own[:, g * HD : (g + 1) * HD], v_own[:, g * HD : (g + 1) * HD]]
    own = jnp.concatenate(parts, axis=1)

    ctx = lax.axis_size("ctx")
    inner, outer = split(ctx)

    def down(k):
        def target(c):
            cz, cy = c // inner, c % inner
            if cz < k - 1:
                return None
            return (cz + 1 if cz < outer - 1 else k - 1) * inner + cy

        return target

    def across(k):
        return lambda c: c ^ 1 if c // inner >= k else None

    def below(k):
        return lambda place: place >= k * inner

    def odd(place):
        return lax.rem(place, 2) == 1

    line, pair = {}, {}

    def send_line(k, value):
        if k < outer:
            line[k] = moved(value, down(k))

    def send_pair(k, value):
        if inner == 2:
            pair[k] = moved(value, across(k))

    send_line(1, own)
    send_pair(0, own)
    state = attend([below(0)], queries, [own], None, rep, ctx == 1)
    for k in range(1, outer):
        send_line(k + 1, line[k])
        send_pair(k, line[k])
        came, wanted = [line[k]], [below(k)]
        if inner == 2:
            came.append(pair[k - 1])
            wanted.append(odd if k == 1 else below(k - 1))
        state = attend(wanted, queries, came, state, rep, inner == 1 and k == outer - 1)
    if inner == 2:
        wanted = [odd if outer == 1 else below(outer - 1)]
        state = attend(wanted, queries, [pair[outer - 1]], state, rep, True)
    return state


def split(ctx):
    inner = 2 if ctx % 2 == 0 else 1
    return inner, ctx // inner


def solution(mesh):
    return jax.shard_map(
        body,
        mesh=mesh,
        in_specs=(P("ctx", "head"), P("ctx", None), P("ctx", None)),
        out_specs=P("ctx", "head"),
        check_vma=False,
    )
```
